32 devices in a mesh: gx: 2 (over x), gy: 4 (over y, core), gz: 4 (over z).
Axes of the slice: x: 2, y: 2, z: 4, core: 2. Of those that a mesh axis runs over, the one named last changes fastest.
Arguments:
- conserved: float32 [5, 16, 32, 256], P(None, 'gz', 'gy', 'gx'), may hold values from -3 to 12, as said below
- metrics: float32 [9, 16, 32, 256], P(None, 'gz', 'gy', 'gx'), may hold values from -0.6 to 2, as said below
- inv_volume: float32 [16, 32, 256], P('gz', 'gy', 'gx'), may hold values from 0.5 to 2
- wake_donor: int32 [256], P('gx'), may hold values from -1 to 255, as said below
Outputs:
- section_state: float32 [5, 16, 32, 256], P(None, 'gz', 'gy', 'gx')
- time_rate: float32 [5, 16, 32, 256], P(None, 'gz', 'gy', 'gx')
The draws below stay inside these ranges and needn't reach their ends.
Inputs may be any that keep to these rules, and one draw needn't show every extreme that they name: `conserved`: each cell holds density rho of 0.5 to 2, pressure p of 0.5 to 2 and velocity components u of -1.5 to 1.5 as (rho, rho u, p / 0.4 + rho |u|^2 / 2). `metrics`: in each cell, row d (entries 3 d to 3 d + 2) has its entry 3 d + d between 0.5 and 2 and its other two entries at most 0.3 times that entry in magnitude. wake_donor[i] is either 256 - 1 - i or -1, and wake_donor[i] >= 0 exactly where wake_donor[255 - i] >= 0.
All inputs are finite; a program needn't handle non-finite values.
Results may differ from the reference program's by a relative error of at most 0.0001.
Values sent between devices are 32-bit elements; how exact they have to be, the bound alone decides.
No kernel may reach another device: no remote copies, remote signals or barrier semaphores. Data moves between devices by JAX's collectives and lax.ppermute only.
A program may use at most 64 MiB of HBM per device.

```python
import math
import jax
import jax.numpy as jnp
from jax import lax

CY = 8
CZ = 4
NX = 256
NY = 32
NZ = 16


def draw_conserved(key, part):
    subkeys = jax.random.split(key, 3)
    grid_shape = (NZ, NY, NX)
    density = jnp.exp(jax.random.uniform(subkeys[0], grid_shape, jnp.float32, -0.6931, 0.6931))
    pressure = jnp.exp(jax.random.uniform(subkeys[1], grid_shape, jnp.float32, -0.6931, 0.6931))
    velocity = jnp.clip(0.5 * jax.random.normal(subkeys[2], (3,) + grid_shape, jnp.float32), -1.5, 1.5)
    energy = pressure / 0.4 + 0.5 * density * jnp.sum(velocity * velocity, axis=0)
    return jnp.concatenate([density[None], density[None] * velocity, energy[None]], axis=0).astype(jnp.float32)


def draw_metrics(key, part):
    subkeys = jax.random.split(key, 2)
    grid_shape = (NZ, NY, NX)
    diagonal = jnp.exp(jax.random.uniform(subkeys[0], (3,) + grid_shape, jnp.float32, -0.6931, 0.6931))
    ratios = jax.random.uniform(subkeys[1], (3, 3) + grid_shape, jnp.float32, -0.3, 0.3)
    entries = []
    for direction in range(3):
        for component in range(3):
            if component == direction:
                entries.append(diagonal[direction])
            else:
                entries.append(ratios[direction, component] * diagonal[direction])
    return jnp.stack(entries).astype(jnp.float32)


def draw_wake_donor(key, part):
    own_key = jax.random.fold_in(key, 4177)
    half_flags = jax.random.randint(own_key, (NX // 2,), 0, 2).astype(jnp.int32)
    flags = jnp.concatenate([half_flags, half_flags[::-1]], axis=0)
    column = jnp.arange(NX, dtype=jnp.int32)
    return jnp.where(flags > 0, NX - 1 - column, -1).astype(jnp.int32)


def steps_of(rng, shape, shards, low, top_value):
    def one(dim, parts):
        steps = jax.random.uniform(jax.random.fold_in(jax.random.fold_in(rng, 6), dim), (parts,), jnp.float32, low / len(shards), top_value / len(shards))
        return jnp.repeat(jnp.exp(steps), shape[dim] // parts).reshape((-1,) + (1,) * (len(shape) - dim - 1))

    gain = one(*shards[0])
    for cut in shards[1:]:
        gain = gain * one(*cut)
    return gain


def setup_inputs(seed: int = 0) -> dict:
    streams_of = jax.random.split(jax.random.key(seed), 5)
    return {
        "conserved": draw_conserved(jax.random.fold_in(streams_of[4], 71), 0),
        "metrics": draw_metrics(jax.random.fold_in(streams_of[4], 71), 0),
        "inv_volume": jnp.clip(jnp.exp(math.log(2.0) - 1.3862944 * jax.random.uniform(streams_of[2], (NZ, NY, NX), jnp.float32) ** steps_of(streams_of[2], (NZ, NY, NX), ((0, 4), (1, 4), (2, 2)), -0.2, 0.2)), 0.5, 2.0),
        "wake_donor": draw_wake_donor(jax.random.fold_in(streams_of[4], 71), 0),
    }


GAMMA = 1.4
WENO_EPS = 1e-06
STEP_SIZE = 0.08

def slab_of(values, start, amount, axis):
    return lax.slice_in_dim(values, start, start + amount, axis=values.ndim + axis)

def cross_of(first, second):
    return [first[1] * second[2] - first[2] * second[1], first[2] * second[0] - first[0] * second[2], first[0] * second[1] - first[1] * second[0]]

def inner_of(first, second):
    return first[0] * second[0] + first[1] * second[1] + first[2] * second[2]

def cell_terms(fields, metric_row):
    density = fields[0]
    velocity = fields[1:4] / density
    kinetic = 0.5 * lax.optimization_barrier(jnp.sum(fields[1:4] * velocity, axis=0))
    pressure = (GAMMA - 1.0) * (fields[4] - kinetic)
    contra = lax.optimization_barrier(jnp.sum(metric_row * velocity, axis=0))
    fluxes = jnp.stack([fields[0] * contra, fields[1] * contra + metric_row[0] * pressure, fields[2] * contra + metric_row[1] * pressure, fields[3] * contra + metric_row[2] * pressure, (fields[4] + pressure) * contra])
    sound_speed = jnp.sqrt(GAMMA * pressure / density)
    speeds = jnp.abs(contra) + sound_speed * jnp.sqrt(lax.optimization_barrier(jnp.sum(metric_row * metric_row, axis=0)))
    primitive = jnp.concatenate([density[None], velocity, pressure[None]], axis=0)
    return (primitive, fluxes, speeds)

def eigen_pair(state, metric_row, pick):
    density = state[0]
    velocity = [state[1], state[2], state[3]]
    pressure = state[4]
    row_size = jnp.sqrt(metric_row[0] ** 2 + metric_row[1] ** 2 + metric_row[2] ** 2)
    normal = [metric_row[member] / row_size for member in range(3)]
    axis_unit = [1.0 if member == pick else 0.0 for member in range(3)]
    raw_cross = cross_of(normal, axis_unit)
    raw_size = jnp.sqrt(raw_cross[0] ** 2 + raw_cross[1] ** 2 + raw_cross[2] ** 2)
    tangent = [raw_cross[member] / raw_size for member in range(3)]
    binormal = cross_of(normal, tangent)
    sound_speed = jnp.sqrt(GAMMA * pressure / density)
    inverse = 1.0 / sound_speed
    kinetic = 0.5 * inner_of(velocity, velocity)
    enthalpy = GAMMA / (GAMMA - 1.0) * pressure / density + kinetic
    normal_speed = inner_of(normal, velocity)
    tangent_speed = inner_of(tangent, velocity)
    binormal_speed = inner_of(binormal, velocity)
    factor = (GAMMA - 1.0) * inverse * inverse
    scaled = factor * kinetic
    left_rows = [[0.5 * (scaled + normal_speed * inverse)] + [0.5 * (-factor * velocity[member] - normal[member] * inverse) for member in range(3)] + [0.5 * factor], [1.0 - scaled] + [factor * velocity[member] for member in range(3)] + [-factor], [-tangent_speed] + tangent + [0.0], [-binormal_speed] + binormal + [0.0], [0.5 * (scaled - normal_speed * inverse)] + [0.5 * (-factor * velocity[member] + normal[member] * inverse) for member in range(3)] + [0.5 * factor]]
    right_columns = [[1.0] + [velocity[member] - sound_speed * normal[member] for member in range(3)] + [enthalpy - sound_speed * normal_speed], [1.0] + velocity + [kinetic], [0.0] + tangent + [tangent_speed], [0.0] + binormal + [binormal_speed], [1.0] + [velocity[member] + sound_speed * normal[member] for member in range(3)] + [enthalpy + sound_speed * normal_speed]]
    return (left_rows, right_columns)

def project_left(matrix, vector):
    return jnp.stack([sum((matrix[member][second] * vector[second] for second in range(5))) for member in range(5)])

def apply_right(matrix, vector):
    return jnp.stack([sum((matrix[second][member] * vector[second] for second in range(5))) for member in range(5)])

def weno_side(stencil):
    far_left, near_left, center, near_right, far_right = stencil
    guess_zero = (2.0 * far_left - 7.0 * near_left + 11.0 * center) / 6.0
    guess_one = (-near_left + 5.0 * center + 2.0 * near_right) / 6.0
    guess_two = (2.0 * center + 5.0 * near_right - far_right) / 6.0
    smooth_zero = 13.0 / 12.0 * (far_left - 2.0 * near_left + center) ** 2 + 0.25 * (far_left - 4.0 * near_left + 3.0 * center) ** 2
    smooth_one = 13.0 / 12.0 * (near_left - 2.0 * center + near_right) ** 2 + 0.25 * (near_left - near_right) ** 2
    smooth_two = 13.0 / 12.0 * (center - 2.0 * near_right + far_right) ** 2 + 0.25 * (3.0 * center - 4.0 * near_right + far_right) ** 2
    weight_zero = 0.1 / (WENO_EPS + smooth_zero) ** 2
    weight_one = 0.6 / (WENO_EPS + smooth_one) ** 2
    weight_two = 0.3 / (WENO_EPS + smooth_two) ** 2
    return (weight_zero * guess_zero + weight_one * guess_one + weight_two * guess_two) / (weight_zero + weight_one + weight_two)

def interface_flux(fields, metric_row, axis, pick):
    primitive, fluxes, speeds = cell_terms(fields, metric_row)
    faces_count = fields.shape[fields.ndim + axis] - 5
    mean_state = 0.5 * (slab_of(primitive, 2, faces_count, axis) + slab_of(primitive, 3, faces_count, axis))
    mean_row = 0.5 * (slab_of(metric_row, 2, faces_count, axis) + slab_of(metric_row, 3, faces_count, axis))
    left_rows, right_columns = eigen_pair(mean_state, mean_row, pick)
    max_speed = slab_of(speeds, 0, faces_count, axis)
    for offset in range(1, 6):
        max_speed = jnp.maximum(max_speed, slab_of(speeds, offset, faces_count, axis))
    upwind = []
    downwind = []
    for offset in range(6):
        state_chars = project_left(left_rows, slab_of(fields, offset, faces_count, axis))
        flux_chars = project_left(left_rows, slab_of(fluxes, offset, faces_count, axis))
        upwind.append(0.5 * (flux_chars + max_speed * state_chars))
        downwind.append(0.5 * (flux_chars - max_speed * state_chars))
    combined = weno_side(upwind[0:5]) + weno_side(downwind[5:0:-1])
    return apply_right(right_columns, combined)

def divergence(fields, metric_row, axis, pick):
    face_flux = interface_flux(fields, metric_row, axis, pick)
    cells_count = face_flux.shape[face_flux.ndim + axis] - 1
    return slab_of(face_flux, 1, cells_count, axis) - slab_of(face_flux, 0, cells_count, axis)

def blocked(fields, metric_row, axis, pick, block_dim, block):
    pieces = fields.shape[block_dim] // block

    def one_block(start):
        flow_part = lax.dynamic_slice_in_dim(fields, start, block, block_dim)
        row_part = lax.dynamic_slice_in_dim(metric_row, start, block, block_dim)
        return divergence(flow_part, row_part, axis, pick)
    starts = jnp.arange(pieces, dtype=jnp.int32) * block
    stacked = lax.map(one_block, starts)
    moved = jnp.moveaxis(stacked, 0, block_dim)
    dims = list(moved.shape)
    merged = dims[:block_dim] + [pieces * block] + dims[block_dim + 2:]
    return moved.reshape(merged)

def reference(conserved, metrics, inv_volume, wake_donor):
    edge_pad = ((0, 0), (0, 0), (0, 0), (3, 3))
    stream_flow = jnp.pad(conserved, edge_pad, mode='edge')
    stream_row = jnp.pad(metrics[0:3], edge_pad, mode='edge')
    momentum_sign = jnp.array([1.0, -1.0, -1.0, -1.0, 1.0], dtype=jnp.float32)[:, None, None, None]
    below_wall = conserved[:, :, 2::-1, :]
    below_row = metrics[3:6, :, 2::-1, :]
    is_wake = wake_donor >= 0
    source_column = jnp.where(is_wake, wake_donor, 0).astype(jnp.int32)
    low_flow = jnp.where(is_wake, jnp.take(below_wall, source_column, axis=3), below_wall * momentum_sign)
    low_row = jnp.where(is_wake, jnp.take(below_row, source_column, axis=3), below_row)
    normal_flow = jnp.concatenate([low_flow, conserved, jnp.repeat(conserved[:, :, -1:, :], 3, axis=2)], axis=2)
    normal_row = jnp.concatenate([low_row, metrics[3:6], jnp.repeat(metrics[3:6, :, -1:, :], 3, axis=2)], axis=2)
    span_flow = jnp.concatenate([conserved[:, -3:], conserved, conserved[:, :3]], axis=1)
    span_metric = metrics[6:9]
    span_row = jnp.concatenate([span_metric[:, -3:], span_metric, span_metric[:, :3]], axis=1)
    summed = blocked(stream_flow, stream_row, -1, 1, 1, CZ)
    summed = summed + blocked(normal_flow, normal_row, -2, 2, 1, CZ)
    summed = summed + blocked(span_flow, span_row, -3, 0, 2, CY)
    time_rate = -inv_volume[None] * summed
    return (conserved + STEP_SIZE * time_rate, time_rate)
```

```python
import functools
import jax
import jax.numpy as jnp
from jax import lax
from jax.experimental import pallas as pl
from jax.experimental.pallas import tpu as pltpu
from jax.sharding import PartitionSpec as P

GAMMA = 1.4
EPS4 = 4e-06
STEP_SIZE = 0.08
SLOT = 32


def cell_terms(q, s):
    inv = 1.0 / q[0]
    u = [q[1] * inv, q[2] * inv, q[3] * inv]
    kinetic = 0.5 * (q[1] * u[0] + q[2] * u[1] + q[3] * u[2])
    p = (GAMMA - 1.0) * (q[4] - kinetic)
    contra = s[0] * u[0] + s[1] * u[1] + s[2] * u[2]
    g = [
        q[0] * contra,
        q[1] * contra + s[0] * p,
        q[2] * contra + s[1] * p,
        q[3] * contra + s[2] * p,
        (q[4] + p) * contra,
    ]
    size = s[0] * s[0] + s[1] * s[1] + s[2] * s[2]
    lam = jnp.abs(contra) + jnp.sqrt(GAMMA * p * inv * size)
    return u, p, g, lam


def correction(d, e1, e2, e3):
    base = d * d + EPS4
    b0 = base + e1 * (4.0 / 3.0 * e1 + d)
    b1 = base + e2 * (4.0 / 3.0 * e2 + d)
    d2 = d + e2
    b2 = (d2 * d2 + EPS4) + e3 * (4.0 / 3.0 * e3 - d2)
    b0 = b0 * b0
    b1 = b1 * b1
    b2 = b2 * b2
    x = b2 + b2
    y = 3.0 * b0
    num = b1 * (x * (e1 - e2) + y * (e2 - e3))
    den = b1 * (b2 + y) + x * y
    return num / den


def face_flux(k, rho, u2, p, a, alpha, eq, eg, dq, dg, gsum):
    i, j = (k + 1) % 3, (k + 2) % 3
    u = [0.5 * v for v in u2]
    flat = a[i] * a[i] + a[j] * a[j]
    rn = lax.rsqrt(flat + a[k] * a[k])
    rt = lax.rsqrt(flat)
    n = [v * rn for v in a]
    li, lj = a[j] * rt, -a[i] * rt
    m = [None] * 3
    m[k] = n[i] * lj - n[j] * li
    m[i] = -n[k] * lj
    m[j] = n[k] * li
    c2 = GAMMA * p / rho
    ic = lax.rsqrt(c2)
    kin = 0.5 * (u[0] * u[0] + u[1] * u[1] + u[2] * u[2])
    hic = 0.5 * ic
    nh = [v * hic for v in n]
    hf = 0.2 * ic * ic

    def project(v):
        w = [v[1] - u[0] * v[0], v[2] - u[1] * v[0], v[3] - u[2] * v[0]]
        t = nh[0] * w[0] + nh[1] * w[1] + nh[2] * w[2]
        z = hf * (v[4] - kin * v[0] - (u[0] * w[0] + u[1] * w[1] + u[2] * w[2]))
        return [
            z - t,
            v[0] - (z + z),
            li * w[i] + lj * w[j],
            m[0] * w[0] + m[1] * w[1] + m[2] * w[2],
            z + t,
        ]

    aq = [[alpha * v for v in e] for e in eq]
    ep = [[eg[r][c] + aq[r][c] for c in range(5)] for r in (0, 1, 2)]
    em = [[eg[r][c] - aq[r][c] for c in range(5)] for r in (3, 2, 1)]
    dp = [dg[0][c] + alpha * dq[0][c] for c in range(5)]
    dm = [alpha * dq[1][c] - dg[1][c] for c in range(5)]
    base = [6.0 * gsum[c] - ep[1][c] - em[1][c] for c in range(5)]
    one = [project(v) for v in (dp, ep[0], ep[1], ep[2])]
    two = [project(v) for v in (dm, em[0], em[1], em[2])]
    w = [
        correction(one[0][c], one[1][c], one[2][c], one[3][c])
        + correction(two[0][c], two[1][c], two[2][c], two[3][c])
        for c in range(5)
    ]
    acoustic = w[0] + w[4]
    total = acoustic + w[1]
    dd = (c2 * ic) * (w[4] - w[0])
    y = [n[0] * dd + m[0] * w[3], n[1] * dd + m[1] * w[3], n[2] * dd + m[2] * w[3]]
    y[i] = y[i] + li * w[2]
    y[j] = y[j] + lj * w[2]
    return [
        base[0] + total,
        base[1] + (u[0] * total + y[0]),
        base[2] + (u[1] * total + y[1]),
        base[3] + (u[2] * total + y[2]),
        base[4]
        + (kin * total + 2.5 * c2 * acoustic + (u[0] * y[0] + u[1] * y[1] + u[2] * y[2])),
    ]


def column_fluxes(cells, k):
    terms = [cell_terms(v[:5], v[5:8]) for v in cells]
    q = [v[:5] for v in cells]
    g = [t[2] for t in terms]
    count = len(cells)
    dq = [[q[r + 1][c] - q[r][c] for c in range(5)] for r in range(count - 1)]
    dg = [[g[r + 1][c] - g[r][c] for c in range(5)] for r in range(count - 1)]
    eq = [None] + [[dq[r][c] - dq[r - 1][c] for c in range(5)] for r in range(1, count - 1)]
    eg = [None] + [[dg[r][c] - dg[r - 1][c] for c in range(5)] for r in range(1, count - 1)]
    pair = [jnp.maximum(terms[r][3], terms[r + 1][3]) for r in range(count - 1)]
    out = []
    for f in range(count - 5):
        one, two = f + 2, f + 3
        alpha = jnp.maximum(jnp.maximum(pair[f], pair[f + 2]), pair[f + 4])
        out.append(
            face_flux(
                k,
                q[one][0] + q[two][0],
                [terms[one][0][c] + terms[two][0][c] for c in range(3)],
                terms[one][1] + terms[two][1],
                [cells[one][5 + c] + cells[two][5 + c] for c in range(3)],
                alpha,
                eq[f + 1 : f + 5],
                eg[f + 1 : f + 5],
                (dq[f + 1], dq[f + 3]),
                (dg[f + 1], dg[f + 3]),
                [g[one][c] + g[two][c] for c in range(5)],
            )
        )
    return out


def lane_flux(fields, k):
    lanes = fields[0].shape[1]

    def ahead(v, by):
        return pltpu.roll(v, (-by) % lanes, 1)

    q, s = fields[:5], fields[5:8]
    u, p, g, lam = cell_terms(q, s)

    def stencil(v):
        nxt = ahead(v, 1)
        d = nxt - v
        prev = ahead(d, -1)
        e = d - prev
        e3 = ahead(e, 1)
        return nxt, (prev, d + e3), (ahead(e, -1), e, e3, ahead(e, 2))

    sq = [stencil(v) for v in q]
    sg = [stencil(v) for v in g]
    pair = jnp.maximum(lam, ahead(lam, 1))
    alpha = jnp.maximum(jnp.maximum(pair, ahead(pair, 2)), ahead(pair, -2))
    return face_flux(
        k,
        q[0] + sq[0][0],
        [v + ahead(v, 1) for v in u],
        p + ahead(p, 1),
        [v + ahead(v, 1) for v in s],
        alpha,
        [[v[2][r] for v in sq] for r in range(4)],
        [[v[2][r] for v in sg] for r in range(4)],
        [[v[1][r] for v in sq] for r in range(2)],
        [[v[1][r] for v in sg] for r in range(2)],
        [g[c] + sg[c][0] for c in range(5)],
    )


def field_of(q_ref, s_ref, d, f, rows):
    return q_ref[f, rows, :] if f < 5 else s_ref[3 * d + f - 5, rows, :]


def iotas(shape):
    return lax.broadcasted_iota(jnp.int32, shape, 0), lax.broadcasted_iota(jnp.int32, shape, 1)


def edge_block(q_ref, s_ref, f, cz, cy, cx):
    _, lane = iotas((cy, cx))
    t = lane & (SLOT - 1)
    index = jnp.where(t < 9, jnp.maximum(t - 3, 0), jnp.minimum(t + (cx - 15), cx - 1))
    block = None
    for z in range(cz):
        part = jnp.take_along_axis(
            field_of(q_ref, s_ref, 0, f, pl.ds(z * cy, cy)), index, axis=1
        )
        block = part if block is None else jnp.where(lane >= z * SLOT, part, block)
    return block


def pack_kernel(dims, q_ref, s_ref, za_ref, zb_ref, ya_ref, yb_ref, x_ref, e_ref):
    cz, cy, cx = dims
    half = cy // 2
    row, lane = iotas((cy, cx))
    even_z = lax.rem(lax.axis_index("gz"), 2) == 0
    gy = lax.axis_index("gy")
    even_y = lax.rem(gy, 2) == 0
    top = (cz - 3) * cy
    first_a = pl.multiple_of(jnp.where(even_z, top, 0), cy)
    first_b = pl.multiple_of(jnp.where(even_z, 0, top), cy)
    for f in range(8):
        za_ref[f] = field_of(q_ref, s_ref, 2, f, pl.ds(first_a, 3 * cy))
        zb_ref[f] = field_of(q_ref, s_ref, 2, f, pl.ds(first_b, 3 * cy))
    even_row = (row & 1) == 0
    for f in range(4):
        for i in range(3):
            low = [field_of(q_ref, s_ref, 1, g, pl.ds(i, cy, stride=half)) for g in (f, f + 4)]
            high = [
                field_of(q_ref, s_ref, 1, g, pl.ds(half - 3 + i, cy, stride=half))
                for g in (f, f + 4)
            ]
            low = jnp.where(even_row, low[0], pltpu.roll(low[1], 1, 0))
            high = jnp.where(even_row, pltpu.roll(high[0], cy - 1, 0), high[1])
            ya_ref[f, pl.ds(i * cy, cy), :] = jnp.where(even_y, high, low)
            flipped = jnp.take_along_axis(low, cx - 1 - lane, axis=1)
            low = jnp.where(gy == 0, flipped, low)
            yb_ref[f, pl.ds(i * cy, cy), :] = jnp.where(even_y, low, high)
    blocks = [edge_block(q_ref, s_ref, f, cz, cy, cx) for f in range(8)]
    lower = (lane & (SLOT - 1)) < SLOT // 2
    for f in range(8):
        e_ref[f] = blocks[f]
    for f in range(4):
        x_ref[f] = jnp.where(lower, blocks[f], pltpu.roll(blocks[f + 4], SLOT // 2, 1))


def main_kernel(dims, nx, *refs):
    cz, cy, cx = dims
    half = cy // 2
    q_ref, s_ref, v_ref, w_ref, e_ref, za_ref, zb_ref, ya_ref, yb_ref, xa_ref = refs[:10]
    xb_ref = refs[10] if nx > 2 else xa_ref
    state_ref, rate_ref, acc_ref = refs[-3:]
    row, lane = iotas((cy, cx))
    gx, gy, gz = lax.axis_index("gx"), lax.axis_index("gy"), lax.axis_index("gz")
    even_x, even_y, even_z = lax.rem(gx, 2) == 0, lax.rem(gy, 2) == 0, lax.rem(gz, 2) == 0
    at_wall = gy == 0
    at_top = gy == lax.axis_size("gy") - 1

    t = lane & (SLOT - 1)
    take_low = jnp.logical_and(t < 3, gx > 0)
    take_high = jnp.logical_and(jnp.logical_and(t >= 15, t < 18), gx < nx - 1)
    ends = []
    for f in range(8):
        xa, xb = xa_ref[f % 4], xb_ref[f % 4]
        low = jnp.where(even_x, xb, xa)
        high = jnp.where(even_x, xa, xb)
        shift_low, shift_high = (-12, 12) if f < 4 else (-28, -4)
        low = pltpu.roll(low, shift_low % cx, 1)
        high = pltpu.roll(high, shift_high % cx, 1)
        ends.append(jnp.where(take_low, low, jnp.where(take_high, high, e_ref[f])))
    edge = lane_flux(ends, 1)
    edge = [v - pltpu.roll(v, 1, 1) for v in edge]
    outer = jnp.logical_or(lane < 3, lane >= cx - 3)
    for z in range(cz):
        rows = pl.ds(z * cy, cy)
        flux = lane_flux([field_of(q_ref, s_ref, 0, f, rows) for f in range(8)], 1)
        index = jnp.where(lane < 3, lane + 3, lane - (cx - 3) + 12)
        index = jnp.where(outer, index + z * SLOT, 0)
        for c in range(5):
            inner = flux[c] - pltpu.roll(flux[c], 1, 1)
            outside = jnp.take_along_axis(edge[c], index, axis=1)
            acc_ref[c, rows, :] = jnp.where(outer, outside, inner)

    cells = []
    for r in range(-3, cz + 3):
        fields = []
        for f in range(8):
            if r < 0:
                rows = pl.ds((r + 3) * cy, cy)
                v = jnp.where(even_z, zb_ref[f, rows, :], za_ref[f, rows, :])
            elif r >= cz:
                rows = pl.ds((r - cz) * cy, cy)
                v = jnp.where(even_z, za_ref[f, rows, :], zb_ref[f, rows, :])
            else:
                v = field_of(q_ref, s_ref, 2, f, pl.ds(r * cy, cy))
            fields.append(v)
        cells.append(fields)
    flux = column_fluxes(cells, 0)
    for z in range(cz):
        rows = pl.ds(z * cy, cy)
        for c in range(5):
            acc_ref[c, rows, :] += flux[z + 1][c] - flux[z][c]

    even_row = (row & 1) == 0
    wake = jnp.broadcast_to(w_ref[...] >= 0, (cy, cx))
    own = [
        [field_of(q_ref, s_ref, 1, f, pl.ds(r, cy, stride=half)) for f in range(8)]
        for r in range(half)
    ]
    low_cells, high_cells = [], []
    for i in range(3):
        low_fields, high_fields = [], []
        for f in range(8):
            rows = pl.ds(i * cy, cy)
            back = pl.ds((2 - i) * cy, cy)
            normal = jnp.where(even_y, yb_ref[f % 4, rows, :], ya_ref[f % 4, rows, :])
            mirror = yb_ref[f % 4, back, :]
            low = jnp.where(at_wall, mirror, normal)
            high = jnp.where(even_y, ya_ref[f % 4, rows, :], yb_ref[f % 4, rows, :])
            if f < 4:
                high = pltpu.roll(high, 1, 0)
            else:
                low = pltpu.roll(low, cy - 1, 0)
            solid = own[2 - i][f]
            solid = -solid if f in (1, 2, 3) else solid
            low = jnp.where(jnp.logical_and(at_wall, jnp.logical_not(wake)), solid, low)
            high = jnp.where(at_top, own[half - 1][f], high)
            low_fields.append(jnp.where(even_row, low, pltpu.roll(own[half - 3 + i][f], 1, 0)))
            high_fields.append(jnp.where(even_row, pltpu.roll(own[i][f], cy - 1, 0), high))
        low_cells.append(low_fields)
        high_cells.append(high_fields)
    flux = column_fluxes(low_cells + own + high_cells, 2)
    for r in range(half):
        rows = pl.ds(r, cy, stride=half)
        scale = v_ref[rows, :] * (-1.0 / 12.0)
        for c in range(5):
            rate = scale * (acc_ref[c, rows, :] + (flux[r + 1][c] - flux[r][c]))
            rate_ref[c, rows, :] = rate
            state_ref[c, rows, :] = own[r][c] + STEP_SIZE * rate


def pairs_of(count, shift, wrap):
    found = []
    for i in range(count):
        j = i + 1 if i % 2 == shift else i - 1
        if wrap:
            j %= count
        if 0 <= j < count:
            found.append((i, j))
    return found


def local(dims, sizes, conserved, metrics, inv_volume, wake_donor):
    cz, cy, cx = dims
    nx, ny, nz = sizes
    q = conserved.reshape(5, cz * cy, cx)
    s = metrics.reshape(9, cz * cy, cx)
    v = inv_volume.reshape(cz * cy, cx)
    w = wake_donor.reshape(1, cx)

    def shape(*d):
        return jax.ShapeDtypeStruct(d, jnp.float32)

    za, zb, ya, yb, x, e = pl.pallas_call(
        functools.partial(pack_kernel, dims),
        out_shape=(
            shape(8, 3 * cy, cx),
            shape(8, 3 * cy, cx),
            shape(4, 3 * cy, cx),
            shape(4, 3 * cy, cx),
            shape(4, cy, cx),
            shape(8, cy, cx),
        ),
        name="pack",
    )(q, s)
    second = []
    for a in range(nx):
        second.append((a * ny, (nx - 1 - a) * ny))
        second += [(a * ny + i, a * ny + j) for i, j in pairs_of(ny, 1, False)]
    za = lax.ppermute(za, "gz", pairs_of(nz, 0, True))
    zb = lax.ppermute(zb, "gz", pairs_of(nz, 1, True))
    ya = lax.ppermute(ya, "gy", pairs_of(ny, 0, False))
    yb = lax.ppermute(yb, ("gx", "gy"), second)
    ends = [lax.ppermute(x, "gx", pairs_of(nx, 0, False))]
    if nx > 2:
        ends.append(lax.ppermute(x, "gx", pairs_of(nx, 1, False)))
    state, rate = pl.pallas_call(
        functools.partial(main_kernel, dims, nx),
        out_shape=(shape(5, cz * cy, cx), shape(5, cz * cy, cx)),
        scratch_shapes=[pltpu.VMEM((5, cz * cy, cx), jnp.float32)],
        name="section",
    )(q, s, v, w, e, za, zb, ya, yb, *ends)
    return state.reshape(conserved.shape), rate.reshape(conserved.shape)


def solution(mesh):
    sizes = (mesh.shape["gx"], mesh.shape["gy"], mesh.shape["gz"])
    placed = (P(None, "gz", "gy", "gx"), P(None, "gz", "gy", "gx"), P("gz", "gy", "gx"), P("gx"))

    def block(conserved, metrics, inv_volume, wake_donor):
        return local(inv_volume.shape, sizes, conserved, metrics, inv_volume, wake_donor)

    return jax.shard_map(
        block,
        mesh=mesh,
        in_specs=placed,
        out_specs=(P(None, "gz", "gy", "gx"), P(None, "gz", "gy", "gx")),
        check_vma=False,
    )
```

```python
import functools
import jax
import jax.numpy as jnp
from jax import lax
from jax.experimental import pallas as pl
from jax.experimental.pallas import tpu as pltpu
from jax.sharding import PartitionSpec as P

GAMMA = 1.4
EPS4 = 4e-06
STEP_SIZE = 0.08
SLOT = 32


def cell_terms(q, s):
    inv = 1.0 / q[0]
    u = [q[1] * inv, q[2] * inv, q[3] * inv]
    kinetic = 0.5 * (q[1] * u[0] + q[2] * u[1] + q[3] * u[2])
    p = (GAMMA - 1.0) * (q[4] - kinetic)
    contra = s[0] * u[0] + s[1] * u[1] + s[2] * u[2]
    g = [
        q[0] * contra,
        q[1] * contra + s[0] * p,
        q[2] * contra + s[1] * p,
        q[3] * contra + s[2] * p,
        (q[4] + p) * contra,
    ]
    size = s[0] * s[0] + s[1] * s[1] + s[2] * s[2]
    lam = jnp.abs(contra) + jnp.sqrt(GAMMA * p * inv * size)
    return u, p, g, lam


def correction(d, e1, e2, e3):
    base = d * d + EPS4
    b0 = base + e1 * (4.0 / 3.0 * e1 + d)
    b1 = base + e2 * (4.0 / 3.0 * e2 + d)
    d2 = d + e2
    b2 = (d2 * d2 + EPS4) + e3 * (4.0 / 3.0 * e3 - d2)
    b0 = b0 * b0
    b1 = b1 * b1
    b2 = b2 * b2
    x = b2 + b2
    y = 3.0 * b0
    num = b1 * (x * (e1 - e2) + y * (e2 - e3))
    den = b1 * (b2 + y) + x * y
    return num / den


def face_flux(k, rho, u2, p, a, alpha, eq, eg, dq, dg, gsum):
    i, j = (k + 1) % 3, (k + 2) % 3
    u = [0.5 * v for v in u2]
    flat = a[i] * a[i] + a[j] * a[j]
    rn = lax.rsqrt(flat + a[k] * a[k])
    rt = lax.rsqrt(flat)
    n = [v * rn for v in a]
    li, lj = a[j] * rt, -a[i] * rt
    m = [None] * 3
    m[k] = n[i] * lj - n[j] * li
    m[i] = -n[k] * lj
    m[j] = n[k] * li
    c2 = GAMMA * p / rho
    ic = lax.rsqrt(c2)
    kin = 0.5 * (u[0] * u[0] + u[1] * u[1] + u[2] * u[2])
    hic = 0.5 * ic
    nh = [v * hic for v in n]
    hf = 0.2 * ic * ic

    def project(v):
        w = [v[1] - u[0] * v[0], v[2] - u[1] * v[0], v[3] - u[2] * v[0]]
        t = nh[0] * w[0] + nh[1] * w[1] + nh[2] * w[2]
        z = hf * (v[4] - kin * v[0] - (u[0] * w[0] + u[1] * w[1] + u[2] * w[2]))
        return [
            z - t,
            v[0] - (z + z),
            li * w[i] + lj * w[j],
            m[0] * w[0] + m[1] * w[1] + m[2] * w[2],
            z + t,
        ]

    aq = [[alpha * v for v in e] for e in eq]
    ep = [[eg[r][c] + aq[r][c] for c in range(5)] for r in (0, 1, 2)]
    em = [[eg[r][c] - aq[r][c] for c in range(5)] for r in (3, 2, 1)]
    dp = [dg[0][c] + alpha * dq[0][c] for c in range(5)]
    dm = [alpha * dq[1][c] - dg[1][c] for c in range(5)]
    base = [6.0 * gsum[c] - ep[1][c] - em[1][c] for c in range(5)]
    one = [project(v) for v in (dp, ep[0], ep[1], ep[2])]
    two = [project(v) for v in (dm, em[0], em[1], em[2])]
    w = [
        correction(one[0][c], one[1][c], one[2][c], one[3][c])
        + correction(two[0][c], two[1][c], two[2][c], two[3][c])
        for c in range(5)
    ]
    acoustic = w[0] + w[4]
    total = acoustic + w[1]
    dd = (c2 * ic) * (w[4] - w[0])
    y = [n[0] * dd + m[0] * w[3], n[1] * dd + m[1] * w[3], n[2] * dd + m[2] * w[3]]
    y[i] = y[i] + li * w[2]
    y[j] = y[j] + lj * w[2]
    return [
        base[0] + total,
        base[1] + (u[0] * total + y[0]),
        base[2] + (u[1] * total + y[1]),
        base[3] + (u[2] * total + y[2]),
        base[4]
        + (kin * total + 2.5 * c2 * acoustic + (u[0] * y[0] + u[1] * y[1] + u[2] * y[2])),
    ]


def column_fluxes(cells, k):
    terms = [cell_terms(v[:5], v[5:8]) for v in cells]
    q = [v[:5] for v in cells]
    g = [t[2] for t in terms]
    count = len(cells)
    dq = [[q[r + 1][c] - q[r][c] for c in range(5)] for r in range(count - 1)]
    dg = [[g[r + 1][c] - g[r][c] for c in range(5)] for r in range(count - 1)]
    eq = [None] + [[dq[r][c] - dq[r - 1][c] for c in range(5)] for r in range(1, count - 1)]
    eg = [None] + [[dg[r][c] - dg[r - 1][c] for c in range(5)] for r in range(1, count - 1)]
    pair = [jnp.maximum(terms[r][3], terms[r + 1][3]) for r in range(count - 1)]
    out = []
    for f in range(count - 5):
        one, two = f + 2, f + 3
        alpha = jnp.maximum(jnp.maximum(pair[f], pair[f + 2]), pair[f + 4])
        out.append(
            face_flux(
                k,
                q[one][0] + q[two][0],
                [terms[one][0][c] + terms[two][0][c] for c in range(3)],
                terms[one][1] + terms[two][1],
                [cells[one][5 + c] + cells[two][5 + c] for c in range(3)],
                alpha,
                eq[f + 1 : f + 5],
                eg[f + 1 : f + 5],
                (dq[f + 1], dq[f + 3]),
                (dg[f + 1], dg[f + 3]),
                [g[one][c] + g[two][c] for c in range(5)],
            )
        )
    return out


def lane_flux(fields, k):
    lanes = fields[0].shape[1]

    def ahead(v, by):
        return pltpu.roll(v, (-by) % lanes, 1)

    q, s = fields[:5], fields[5:8]
    u, p, g, lam = cell_terms(q, s)

    def stencil(v):
        nxt = ahead(v, 1)
        d = nxt - v
        prev = ahead(d, -1)
        e = d - prev
        e3 = ahead(e, 1)
        return nxt, (prev, d + e3), (ahead(e, -1), e, e3, ahead(e, 2))

    sq = [stencil(v) for v in q]
    sg = [stencil(v) for v in g]
    pair = jnp.maximum(lam, ahead(lam, 1))
    alpha = jnp.maximum(jnp.maximum(pair, ahead(pair, 2)), ahead(pair, -2))
    return face_flux(
        k,
        q[0] + sq[0][0],
        [v + ahead(v, 1) for v in u],
        p + ahead(p, 1),
        [v + ahead(v, 1) for v in s],
        alpha,
        [[v[2][r] for v in sq] for r in range(4)],
        [[v[2][r] for v in sg] for r in range(4)],
        [[v[1][r] for v in sq] for r in range(2)],
        [[v[1][r] for v in sg] for r in range(2)],
        [g[c] + sg[c][0] for c in range(5)],
    )


def field_of(q_ref, s_ref, d, f, rows):
    return q_ref[f, rows, :] if f < 5 else s_ref[3 * d + f - 5, rows, :]


def iotas(shape):
    return lax.broadcasted_iota(jnp.int32, shape, 0), lax.broadcasted_iota(jnp.int32, shape, 1)


def edge_block(q_ref, s_ref, f, cz, cy, cx):
    _, lane = iotas((cy, cx))
    t = lane & (SLOT - 1)
    index = jnp.where(t < 9, jnp.maximum(t - 3, 0), jnp.minimum(t + (cx - 15), cx - 1))
    block = None
    for z in range(cz):
        part = jnp.take_along_axis(
            field_of(q_ref, s_ref, 0, f, pl.ds(z * cy, cy)), index, axis=1
        )
        block = part if block is None else jnp.where(lane >= z * SLOT, part, block)
    return block


def pack_kernel(dims, q_ref, s_ref, za_ref, zb_ref, ya_ref, yb_ref, x_ref, e_ref):
    cz, cy, cx = dims
    half = cy // 2
    row, lane = iotas((cy, cx))
    even_z = lax.rem(lax.axis_index("gz"), 2) == 0
    gy = lax.axis_index("gy")
    even_y = lax.rem(gy, 2) == 0
    top = (cz - 3) * cy
    first_a = pl.multiple_of(jnp.where(even_z, top, 0), cy)
    first_b = pl.multiple_of(jnp.where(even_z, 0, top), cy)
    for f in range(8):
        za_ref[f] = field_of(q_ref, s_ref, 2, f, pl.ds(first_a, 3 * cy))
        zb_ref[f] = field_of(q_ref, s_ref, 2, f, pl.ds(first_b, 3 * cy))
    even_row = (row & 1) == 0
    for f in range(4):
        for i in range(3):
            low = [field_of(q_ref, s_ref, 1, g, pl.ds(i, cy, stride=half)) for g in (f, f + 4)]
            high = [
                field_of(q_ref, s_ref, 1, g, pl.ds(half - 3 + i, cy, stride=half))
                for g in (f, f + 4)
            ]
            low = jnp.where(even_row, low[0], pltpu.roll(low[1], 1, 0))
            high = jnp.where(even_row, pltpu.roll(high[0], cy - 1, 0), high[1])
            ya_ref[f, pl.ds(i * cy, cy), :] = jnp.where(even_y, high, low)
            flipped = jnp.take_along_axis(low, cx - 1 - lane, axis=1)
            low = jnp.where(gy == 0, flipped, low)
            yb_ref[f, pl.ds(i * cy, cy), :] = jnp.where(even_y, low, high)
    blocks = [edge_block(q_ref, s_ref, f, cz, cy, cx) for f in range(8)]
    lower = (lane & (SLOT - 1)) < SLOT // 2
    for f in range(8):
        e_ref[f] = blocks[f]
    for f in range(4):
        x_ref[f] = jnp.where(lower, blocks[f], pltpu.roll(blocks[f + 4], SLOT // 2, 1))


def main_kernel(dims, nx, *refs):
    cz, cy, cx = dims
    half = cy // 2
    q_ref, s_ref, v_ref, w_ref, e_ref, za_ref, zb_ref, ya_ref, yb_ref, xa_ref = refs[:10]
    xb_ref = refs[10] if nx > 2 else xa_ref
    state_ref, rate_ref, acc_ref = refs[-3:]
    row, lane = iotas((cy, cx))
    gx, gy, gz = lax.axis_index("gx"), lax.axis_index("gy"), lax.axis_index("gz")
    even_x, even_y, even_z = lax.rem(gx, 2) == 0, lax.rem(gy, 2) == 0, lax.rem(gz, 2) == 0
    at_wall = gy == 0
    at_top = gy == lax.axis_size("gy") - 1

    t = lane & (SLOT - 1)
    take_low = jnp.logical_and(t < 3, gx > 0)
    take_high = jnp.logical_and(jnp.logical_and(t >= 15, t < 18), gx < nx - 1)
    ends = []
    for f in range(8):
        xa, xb = xa_ref[f % 4], xb_ref[f % 4]
        low = jnp.where(even_x, xb, xa)
        high = jnp.where(even_x, xa, xb)
        shift_low, shift_high = (-12, 12) if f < 4 else (-28, -4)
        low = pltpu.roll(low, shift_low % cx, 1)
        high = pltpu.roll(high, shift_high % cx, 1)
        ends.append(jnp.where(take_low, low, jnp.where(take_high, high, e_ref[f])))
    edge = lane_flux(ends, 1)
    edge = [v - pltpu.roll(v, 1, 1) for v in edge]
    outer = jnp.logical_or(lane < 3, lane >= cx - 3)
    for z in range(cz):
        rows = pl.ds(z * cy, cy)
        flux = lane_flux([field_of(q_ref, s_ref, 0, f, rows) for f in range(8)], 1)
        index = jnp.where(lane < 3, lane + 3, lane - (cx - 3) + 12)
        index = jnp.where(outer, index + z * SLOT, 0)
        for c in range(5):
            inner = flux[c] - pltpu.roll(flux[c], 1, 1)
            outside = jnp.take_along_axis(edge[c], index, axis=1)
            acc_ref[c, rows, :] = jnp.where(outer, outside, inner)

    cells = []
    for r in range(-3, cz + 3):
        fields = []
        for f in range(8):
            if r < 0:
                rows = pl.ds((r + 3) * cy, cy)
                v = jnp.where(even_z, zb_ref[f, rows, :], za_ref[f, rows, :])
            elif r >= cz:
                rows = pl.ds((r - cz) * cy, cy)
                v = jnp.where(even_z, za_ref[f, rows, :], zb_ref[f, rows, :])
            else:
                v = field_of(q_ref, s_ref, 2, f, pl.ds(r * cy, cy))
            fields.append(v)
        cells.append(fields)
    flux = column_fluxes(cells, 0)
    for z in range(cz):
        rows = pl.ds(z * cy, cy)
        for c in range(5):
            acc_ref[c, rows, :] += flux[z + 1][c] - flux[z][c]

    even_row = (row & 1) == 0
    wake = jnp.broadcast_to(w_ref[...] >= 0, (cy, cx))
    own = [
        [field_of(q_ref, s_ref, 1, f, pl.ds(r, cy, stride=half)) for f in range(8)]
        for r in range(half)
    ]
    low_cells, high_cells = [], []
    for i in range(3):
        low_fields, high_fields = [], []
        for f in range(8):
            rows = pl.ds(i * cy, cy)
            back = pl.ds((2 - i) * cy, cy)
            normal = jnp.where(even_y, yb_ref[f % 4, rows, :], ya_ref[f % 4, rows, :])
            mirror = yb_ref[f % 4, back, :]
            low = jnp.where(at_wall, mirror, normal)
            high = jnp.where(even_y, ya_ref[f % 4, rows, :], yb_ref[f % 4, rows, :])
            if f < 4:
                high = pltpu.roll(high, 1, 0)
            else:
                low = pltpu.roll(low, cy - 1, 0)
            solid = own[2 - i][f]
            solid = -solid if f in (1, 2, 3) else solid
            low = jnp.where(jnp.logical_and(at_wall, jnp.logical_not(wake)), solid, low)
            high = jnp.where(at_top, own[half - 1][f], high)
            low_fields.append(jnp.where(even_row, low, pltpu.roll(own[half - 3 + i][f], 1, 0)))
            high_fields.append(jnp.where(even_row, pltpu.roll(own[i][f], cy - 1, 0), high))
        low_cells.append(low_fields)
        high_cells.append(high_fields)
    flux = column_fluxes(low_cells + own + high_cells, 2)
    for r in range(half):
        rows = pl.ds(r, cy, stride=half)
        scale = v_ref[rows, :] * (-1.0 / 12.0)
        for c in range(5):
            rate = scale * (acc_ref[c, rows, :] + (flux[r + 1][c] - flux[r][c]))
            rate_ref[c, rows, :] = rate
            state_ref[c, rows, :] = own[r][c] + STEP_SIZE * rate


def pairs_of(count, shift, wrap):
    found = []
    for i in range(count):
        j = i + 1 if i % 2 == shift else i - 1
        if wrap:
            j %= count
        if 0 <= j < count:
            found.append((i, j))
    return found


def local(dims, sizes, conserved, metrics, inv_volume, wake_donor):
    cz, cy, cx = dims
    nx, ny, nz = sizes
    q = conserved.reshape(5, cz * cy, cx)
    s = metrics.reshape(9, cz * cy, cx)
    v = inv_volume.reshape(cz * cy, cx)
    w = wake_donor.reshape(1, cx)

    def shape(*d):
        return jax.ShapeDtypeStruct(d, jnp.float32)

    za, zb, ya, yb, x, e = pl.pallas_call(
        functools.partial(pack_kernel, dims),
        out_shape=(
            shape(8, 3 * cy, cx),
            shape(8, 3 * cy, cx),
            shape(4, 3 * cy, cx),
            shape(4, 3 * cy, cx),
            shape(4, cy, cx),
            shape(8, cy, cx),
        ),
        compiler_params=pltpu.CompilerParams(vmem_limit_bytes=4 * 2**20),
        name="pack",
    )(q, s)
    second = []
    for a in range(nx):
        second.append((a * ny, (nx - 1 - a) * ny))
        second += [(a * ny + i, a * ny + j) for i, j in pairs_of(ny, 1, False)]
    za = lax.ppermute(za, "gz", pairs_of(nz, 0, True))
    zb = lax.ppermute(zb, "gz", pairs_of(nz, 1, True))
    ya = lax.ppermute(ya, "gy", pairs_of(ny, 0, False))
    yb = lax.ppermute(yb, ("gx", "gy"), second)
    ends = [lax.ppermute(x, "gx", pairs_of(nx, 0, False))]
    if nx > 2:
        ends.append(lax.ppermute(x, "gx", pairs_of(nx, 1, False)))
    state, rate = pl.pallas_call(
        functools.partial(main_kernel, dims, nx),
        out_shape=(shape(5, cz * cy, cx), shape(5, cz * cy, cx)),
        scratch_shapes=[pltpu.VMEM((5, cz * cy, cx), jnp.float32)],
        compiler_params=pltpu.CompilerParams(vmem_limit_bytes=8 * 2**20),
        name="section",
    )(q, s, v, w, e, za, zb, ya, yb, *ends)
    return state.reshape(conserved.shape), rate.reshape(conserved.shape)


def solution(mesh):
    sizes = (mesh.shape["gx"], mesh.shape["gy"], mesh.shape["gz"])
    placed = (P(None, "gz", "gy", "gx"), P(None, "gz", "gy", "gx"), P("gz", "gy", "gx"), P("gx"))

    def block(conserved, metrics, inv_volume, wake_donor):
        return local(inv_volume.shape, sizes, conserved, metrics, inv_volume, wake_donor)

    return jax.shard_map(
        block,
        mesh=mesh,
        in_specs=placed,
        out_specs=(P(None, "gz", "gy", "gx"), P(None, "gz", "gy", "gx")),
        check_vma=False,
    )
```

```python
import functools
import jax
import jax.numpy as jnp
from jax import lax
from jax.experimental import pallas as pl
from jax.experimental.pallas import tpu as pltpu
from jax.sharding import PartitionSpec as P

GAMMA = 1.4
EPS4 = 4e-06
STEP_SIZE = 0.08
SLOT = 32
VMEM_LIMIT = 4 * 2**20


def cell_terms(q, s):
    inv = 1.0 / q[0]
    u = [q[1] * inv, q[2] * inv, q[3] * inv]
    kinetic = 0.5 * (q[1] * u[0] + q[2] * u[1] + q[3] * u[2])
    p = (GAMMA - 1.0) * (q[4] - kinetic)
    contra = s[0] * u[0] + s[1] * u[1] + s[2] * u[2]
    g = [
        q[0] * contra,
        q[1] * contra + s[0] * p,
        q[2] * contra + s[1] * p,
        q[3] * contra + s[2] * p,
        (q[4] + p) * contra,
    ]
    size = s[0] * s[0] + s[1] * s[1] + s[2] * s[2]
    lam = jnp.abs(contra) + jnp.sqrt(GAMMA * p * inv * size)
    return u, p, g, lam


def correction(d, e1, e2, e3):
    base = d * d + EPS4
    b0 = base + e1 * (4.0 / 3.0 * e1 + d)
    b1 = base + e2 * (4.0 / 3.0 * e2 + d)
    d2 = d + e2
    b2 = (d2 * d2 + EPS4) + e3 * (4.0 / 3.0 * e3 - d2)
    b0 = b0 * b0
    b1 = b1 * b1
    b2 = b2 * b2
    x = b2 + b2
    y = 3.0 * b0
    num = b1 * (x * (e1 - e2) + y * (e2 - e3))
    den = b1 * (b2 + y) + x * y
    return num / den


def face_flux(k, rho, u2, p, a, alpha, eq, eg, dq, dg, gsum):
    i, j = (k + 1) % 3, (k + 2) % 3
    u = [0.5 * v for v in u2]
    flat = a[i] * a[i] + a[j] * a[j]
    rn = lax.rsqrt(flat + a[k] * a[k])
    rt = lax.rsqrt(flat)
    n = [v * rn for v in a]
    li, lj = a[j] * rt, -a[i] * rt
    m = [None] * 3
    m[k] = n[i] * lj - n[j] * li
    m[i] = -n[k] * lj
    m[j] = n[k] * li
    c2 = GAMMA * p / rho
    ic = lax.rsqrt(c2)
    kin = 0.5 * (u[0] * u[0] + u[1] * u[1] + u[2] * u[2])
    hic = 0.5 * ic
    nh = [v * hic for v in n]
    hf = 0.2 * ic * ic

    def project(v):
        w = [v[1] - u[0] * v[0], v[2] - u[1] * v[0], v[3] - u[2] * v[0]]
        t = nh[0] * w[0] + nh[1] * w[1] + nh[2] * w[2]
        z = hf * (v[4] - kin * v[0] - (u[0] * w[0] + u[1] * w[1] + u[2] * w[2]))
        return [
            z - t,
            v[0] - (z + z),
            li * w[i] + lj * w[j],
            m[0] * w[0] + m[1] * w[1] + m[2] * w[2],
            z + t,
        ]

    aq = [[alpha * v for v in e] for e in eq]
    ep = [[eg[r][c] + aq[r][c] for c in range(5)] for r in (0, 1, 2)]
    em = [[eg[r][c] - aq[r][c] for c in range(5)] for r in (3, 2, 1)]
    dp = [dg[0][c] + alpha * dq[0][c] for c in range(5)]
    dm = [alpha * dq[1][c] - dg[1][c] for c in range(5)]
    base = [6.0 * gsum[c] - ep[1][c] - em[1][c] for c in range(5)]
    one = [project(v) for v in (dp, ep[0], ep[1], ep[2])]
    two = [project(v) for v in (dm, em[0], em[1], em[2])]
    w = [
        correction(one[0][c], one[1][c], one[2][c], one[3][c])
        + correction(two[0][c], two[1][c], two[2][c], two[3][c])
        for c in range(5)
    ]
    acoustic = w[0] + w[4]
    total = acoustic + w[1]
    dd = (c2 * ic) * (w[4] - w[0])
    y = [n[0] * dd + m[0] * w[3], n[1] * dd + m[1] * w[3], n[2] * dd + m[2] * w[3]]
    y[i] = y[i] + li * w[2]
    y[j] = y[j] + lj * w[2]
    return [
        base[0] + total,
        base[1] + (u[0] * total + y[0]),
        base[2] + (u[1] * total + y[1]),
        base[3] + (u[2] * total + y[2]),
        base[4]
        + (kin * total + 2.5 * c2 * acoustic + (u[0] * y[0] + u[1] * y[1] + u[2] * y[2])),
    ]


def column_fluxes(cells, k):
    terms = [cell_terms(v[:5], v[5:8]) for v in cells]
    q = [v[:5] for v in cells]
    g = [t[2] for t in terms]
    count = len(cells)
    dq = [[q[r + 1][c] - q[r][c] for c in range(5)] for r in range(count - 1)]
    dg = [[g[r + 1][c] - g[r][c] for c in range(5)] for r in range(count - 1)]
    eq = [None] + [[dq[r][c] - dq[r - 1][c] for c in range(5)] for r in range(1, count - 1)]
    eg = [None] + [[dg[r][c] - dg[r - 1][c] for c in range(5)] for r in range(1, count - 1)]
    pair = [jnp.maximum(terms[r][3], terms[r + 1][3]) for r in range(count - 1)]
    out = []
    for f in range(count - 5):
        one, two = f + 2, f + 3
        alpha = jnp.maximum(jnp.maximum(pair[f], pair[f + 2]), pair[f + 4])
        out.append(
            face_flux(
                k,
                q[one][0] + q[two][0],
                [terms[one][0][c] + terms[two][0][c] for c in range(3)],
                terms[one][1] + terms[two][1],
                [cells[one][5 + c] + cells[two][5 + c] for c in range(3)],
                alpha,
                eq[f + 1 : f + 5],
                eg[f + 1 : f + 5],
                (dq[f + 1], dq[f + 3]),
                (dg[f + 1], dg[f + 3]),
                [g[one][c] + g[two][c] for c in range(5)],
            )
        )
    return out


def lane_flux(fields, k):
    lanes = fields[0].shape[1]

    def ahead(v, by):
        return pltpu.roll(v, (-by) % lanes, 1)

    q, s = fields[:5], fields[5:8]
    u, p, g, lam = cell_terms(q, s)

    def stencil(v):
        nxt = ahead(v, 1)
        d = nxt - v
        prev = ahead(d, -1)
        e = d - prev
        e3 = ahead(e, 1)
        return nxt, (prev, d + e3), (ahead(e, -1), e, e3, ahead(e, 2))

    sq = [stencil(v) for v in q]
    sg = [stencil(v) for v in g]
    pair = jnp.maximum(lam, ahead(lam, 1))
    alpha = jnp.maximum(jnp.maximum(pair, ahead(pair, 2)), ahead(pair, -2))
    return face_flux(
        k,
        q[0] + sq[0][0],
        [v + ahead(v, 1) for v in u],
        p + ahead(p, 1),
        [v + ahead(v, 1) for v in s],
        alpha,
        [[v[2][r] for v in sq] for r in range(4)],
        [[v[2][r] for v in sg] for r in range(4)],
        [[v[1][r] for v in sq] for r in range(2)],
        [[v[1][r] for v in sg] for r in range(2)],
        [g[c] + sg[c][0] for c in range(5)],
    )


def field_of(q_ref, s_ref, d, f, rows):
    return q_ref[f, rows, :] if f < 5 else s_ref[3 * d + f - 5, rows, :]


def iotas(shape):
    return lax.broadcasted_iota(jnp.int32, shape, 0), lax.broadcasted_iota(jnp.int32, shape, 1)


def edge_block(q_ref, s_ref, f, cz, cy, cx):
    _, lane = iotas((cy, cx))
    t = lane & (SLOT - 1)
    index = jnp.where(t < 9, jnp.maximum(t - 3, 0), jnp.minimum(t + (cx - 15), cx - 1))
    block = None
    for z in range(cz):
        part = jnp.take_along_axis(
            field_of(q_ref, s_ref, 0, f, pl.ds(z * cy, cy)), index, axis=1
        )
        block = part if block is None else jnp.where(lane >= z * SLOT, part, block)
    return block


def pack_kernel(dims, *refs):
    cz, cy, cx = dims
    q_hbm, s_hbm, v_hbm, w_hbm = refs[:4]
    q_ref, s_ref, v_ref, w_ref, za_ref, zb_ref, ya_ref, yb_ref, x_ref, e_ref = refs[4:14]
    sems = refs[14]
    loads = [
        pltpu.make_async_copy(source, target, sems.at[i])
        for i, (source, target) in enumerate(
            ((q_hbm, q_ref), (s_hbm, s_ref), (v_hbm, v_ref), (w_hbm, w_ref))
        )
    ]
    for load in loads:
        load.start()
    half = cy // 2
    row, lane = iotas((cy, cx))
    even_z = lax.rem(lax.axis_index("gz"), 2) == 0
    gy = lax.axis_index("gy")
    even_y = lax.rem(gy, 2) == 0
    top = (cz - 3) * cy
    first_a = pl.multiple_of(jnp.where(even_z, top, 0), cy)
    first_b = pl.multiple_of(jnp.where(even_z, 0, top), cy)
    for load in loads:
        load.wait()
    for f in range(8):
        za_ref[f] = field_of(q_ref, s_ref, 2, f, pl.ds(first_a, 3 * cy))
        zb_ref[f] = field_of(q_ref, s_ref, 2, f, pl.ds(first_b, 3 * cy))
    even_row = (row & 1) == 0
    for f in range(4):
        for i in range(3):
            low = [field_of(q_ref, s_ref, 1, g, pl.ds(i, cy, stride=half)) for g in (f, f + 4)]
            high = [
                field_of(q_ref, s_ref, 1, g, pl.ds(half - 3 + i, cy, stride=half))
                for g in (f, f + 4)
            ]
            low = jnp.where(even_row, low[0], pltpu.roll(low[1], 1, 0))
            high = jnp.where(even_row, pltpu.roll(high[0], cy - 1, 0), high[1])
            ya_ref[f, pl.ds(i * cy, cy), :] = jnp.where(even_y, high, low)
            flipped = jnp.take_along_axis(low, cx - 1 - lane, axis=1)
            low = jnp.where(gy == 0, flipped, low)
            yb_ref[f, pl.ds(i * cy, cy), :] = jnp.where(even_y, low, high)
    blocks = [edge_block(q_ref, s_ref, f, cz, cy, cx) for f in range(8)]
    lower = (lane & (SLOT - 1)) < SLOT // 2
    for f in range(8):
        e_ref[f] = blocks[f]
    for f in range(4):
        x_ref[f] = jnp.where(lower, blocks[f], pltpu.roll(blocks[f + 4], SLOT // 2, 1))


def stream_inner(dims, r):
    cz, cy, cx = dims
    for z in range(cz):
        rows = pl.ds(z * cy, cy)
        flux = lane_flux([field_of(r["q"], r["s"], 0, f, rows) for f in range(8)], 1)
        for c in range(5):
            r["out"][c, rows, :] = flux[c] - pltpu.roll(flux[c], 1, 1)


def span(dims, r):
    cz, cy, cx = dims
    even_z = lax.rem(lax.axis_index("gz"), 2) == 0
    cells = []
    for k in range(-3, cz + 3):
        fields = []
        for f in range(8):
            if k < 0:
                rows = pl.ds((k + 3) * cy, cy)
                v = jnp.where(even_z, r["zb"][f, rows, :], r["za"][f, rows, :])
            elif k >= cz:
                rows = pl.ds((k - cz) * cy, cy)
                v = jnp.where(even_z, r["za"][f, rows, :], r["zb"][f, rows, :])
            else:
                v = field_of(r["q"], r["s"], 2, f, pl.ds(k * cy, cy))
            fields.append(v)
        cells.append(fields)
    flux = column_fluxes(cells, 0)
    for z in range(cz):
        rows = pl.ds(z * cy, cy)
        for c in range(5):
            r["out"][c, rows, :] = flux[z + 1][c] - flux[z][c]


def normal(dims, r):
    cz, cy, cx = dims
    half = cy // 2
    row, _ = iotas((cy, cx))
    gy = lax.axis_index("gy")
    even_y = lax.rem(gy, 2) == 0
    at_wall = gy == 0
    at_top = gy == lax.axis_size("gy") - 1
    even_row = (row & 1) == 0
    wake = jnp.broadcast_to(r["w"][...] >= 0, (cy, cx))
    walled = jnp.logical_and(at_wall, jnp.logical_not(wake))
    ya, yb = r["ya"], r["yb"]
    own = [
        [field_of(r["q"], r["s"], 1, f, pl.ds(i, cy, stride=half)) for f in range(8)]
        for i in range(half)
    ]
    low_cells, high_cells = [], []
    for i in range(3):
        low_fields, high_fields = [], []
        for f in range(8):
            rows = pl.ds(i * cy, cy)
            back = pl.ds((2 - i) * cy, cy)
            low = jnp.where(even_y, yb[f % 4, rows, :], ya[f % 4, rows, :])
            low = jnp.where(at_wall, yb[f % 4, back, :], low)
            high = jnp.where(even_y, ya[f % 4, rows, :], yb[f % 4, rows, :])
            if f < 4:
                high = pltpu.roll(high, 1, 0)
            else:
                low = pltpu.roll(low, cy - 1, 0)
            solid = own[2 - i][f]
            solid = -solid if f in (1, 2, 3) else solid
            low = jnp.where(walled, solid, low)
            high = jnp.where(at_top, own[half - 1][f], high)
            low_fields.append(jnp.where(even_row, low, pltpu.roll(own[half - 3 + i][f], 1, 0)))
            high_fields.append(jnp.where(even_row, pltpu.roll(own[i][f], cy - 1, 0), high))
        low_cells.append(low_fields)
        high_cells.append(high_fields)
    flux = column_fluxes(low_cells + own + high_cells, 2)
    for i in range(half):
        rows = pl.ds(i, cy, stride=half)
        for c in range(5):
            r["out"][c, rows, :] = r["acc"][c, rows, :] + (flux[i + 1][c] - flux[i][c])


def stream_ends(dims, r):
    cz, cy, cx = dims
    _, lane = iotas((cy, cx))
    gx = lax.axis_index("gx")
    even_x = lax.rem(gx, 2) == 0
    t = lane & (SLOT - 1)
    take_low = jnp.logical_and(t < 3, gx > 0)
    inside = gx < lax.axis_size("gx") - 1
    take_high = jnp.logical_and(jnp.logical_and(t >= 15, t < 18), inside)
    xa_ref = r["xa"]
    xb_ref = r.get("xb", xa_ref)
    ends = []
    for f in range(8):
        xa, xb = xa_ref[f % 4], xb_ref[f % 4]
        low = jnp.where(even_x, xb, xa)
        high = jnp.where(even_x, xa, xb)
        shift_low, shift_high = (-12, 12) if f < 4 else (-28, -4)
        low = pltpu.roll(low, shift_low % cx, 1)
        high = pltpu.roll(high, shift_high % cx, 1)
        ends.append(jnp.where(take_low, low, jnp.where(take_high, high, r["e"][f])))
    edge = lane_flux(ends, 1)
    return [v - pltpu.roll(v, 1, 1) for v in edge]


def finish(dims, r):
    cz, cy, cx = dims
    edge = stream_ends(dims, r)
    _, lane = iotas((cy, cx))
    outer = jnp.logical_or(lane < 3, lane >= cx - 3)
    index = jnp.where(lane < 3, lane + 3, lane - (cx - 3) + 12)
    for z in range(cz):
        rows = pl.ds(z * cy, cy)
        scale = r["v"][rows, :] * (-1.0 / 12.0)
        spot = jnp.where(outer, index + z * SLOT, 0)
        for c in range(5):
            ends = jnp.take_along_axis(edge[c], spot, axis=1)
            rate = scale * (r["acc"][c, rows, :] + jnp.where(outer, ends, r["inner"][c, rows, :]))
            r["rate"][c, rows, :] = rate
            r["state"][c, rows, :] = r["q"][c, rows, :] + STEP_SIZE * rate


def pairs_of(count, shift, wrap):
    found = []
    for i in range(count):
        j = i + 1 if i % 2 == shift else i - 1
        if wrap:
            j %= count
        if 0 <= j < count:
            found.append((i, j))
    return found


def stage(body, dims, inputs, outputs, flops):
    names = tuple(inputs) + tuple(outputs)

    def kernel(*refs):
        body(dims, dict(zip(names, refs)))

    moved = 4 * sum(v.size for v in tuple(inputs.values()) + tuple(outputs.values()))
    return pl.pallas_call(
        kernel,
        out_shape=tuple(outputs.values()),
        compiler_params=pltpu.CompilerParams(vmem_limit_bytes=VMEM_LIMIT),
        cost_estimate=pl.CostEstimate(flops=flops, bytes_accessed=moved, transcendentals=0),
        name=body.__name__,
    )(*inputs.values())


def local(dims, sizes, conserved, metrics, inv_volume, wake_donor):
    cz, cy, cx = dims
    nx, ny, nz = sizes
    q = conserved.reshape(5, cz * cy, cx)
    s = metrics.reshape(9, cz * cy, cx)
    v = inv_volume.reshape(cz * cy, cx)
    w = wake_donor.reshape(1, cx)

    def shape(*d):
        return jax.ShapeDtypeStruct(d, jnp.float32)

    q, s, v, w, za, zb, ya, yb, x, e = pl.pallas_call(
        functools.partial(pack_kernel, dims),
        in_specs=[pl.BlockSpec(memory_space=pltpu.HBM)] * 4,
        out_shape=(
            shape(*q.shape),
            shape(*s.shape),
            shape(*v.shape),
            jax.ShapeDtypeStruct(w.shape, w.dtype),
            shape(8, 3 * cy, cx),
            shape(8, 3 * cy, cx),
            shape(4, 3 * cy, cx),
            shape(4, 3 * cy, cx),
            shape(4, cy, cx),
            shape(8, cy, cx),
        ),
        scratch_shapes=[pltpu.SemaphoreType.DMA((4,))],
        compiler_params=pltpu.CompilerParams(vmem_limit_bytes=VMEM_LIMIT),
        name="pack",
    )(*[pltpu.with_memory_space_constraint(t, pltpu.HBM) for t in (q, s, v, w)])
    second = []
    for a in range(nx):
        second.append((a * ny, (nx - 1 - a) * ny))
        second += [(a * ny + i, a * ny + j) for i, j in pairs_of(ny, 1, False)]
    za = lax.ppermute(za, "gz", pairs_of(nz, 0, True))
    zb = lax.ppermute(zb, "gz", pairs_of(nz, 1, True))
    ya = lax.ppermute(ya, "gy", pairs_of(ny, 0, False))
    yb = lax.ppermute(yb, ("gx", "gy"), second)
    ends = {"xa": lax.ppermute(x, "gx", pairs_of(nx, 0, False))}
    if nx > 2:
        ends["xb"] = lax.ppermute(x, "gx", pairs_of(nx, 1, False))
    total = {"out": shape(*q.shape)}
    work = cz * cy * cx * 4000
    (inner,) = stage(stream_inner, dims, {"q": q, "s": s}, total, work)
    zero = {"q": q, "s": s, "za": za, "zb": zb}
    (acc,) = stage(span, dims, zero, total, work)
    one = {"q": q, "s": s, "w": w, "ya": ya, "yb": yb, "acc": acc}
    (acc,) = stage(normal, dims, one, total, work)
    two = {"q": q, "v": v, "e": e, "acc": acc, "inner": inner, **ends}
    outs = {"state": shape(*q.shape), "rate": shape(*q.shape)}
    state, rate = stage(finish, dims, two, outs, work)
    return state.reshape(conserved.shape), rate.reshape(conserved.shape)


def solution(mesh):
    sizes = (mesh.shape["gx"], mesh.shape["gy"], mesh.shape["gz"])
    placed = (P(None, "gz", "gy", "gx"), P(None, "gz", "gy", "gx"), P("gz", "gy", "gx"), P("gx"))

    def block(conserved, metrics, inv_volume, wake_donor):
        return local(inv_volume.shape, sizes, conserved, metrics, inv_volume, wake_donor)

    return jax.shard_map(
        block,
        mesh=mesh,
        in_specs=placed,
        out_specs=(P(None, "gz", "gy", "gx"), P(None, "gz", "gy", "gx")),
        check_vma=False,
    )
```
